32 devices in a mesh: groups: 2 (over x), seq: 8 (over z, y), dec: 2 (over core).
Axes of the slice: x: 2, y: 2, z: 4, core: 2. Of those that a mesh axis runs over, the one named last changes fastest.
Arguments:
- tokens: bfloat16 [2048, 4096], P(('groups', 'seq')), parts along dimension 0, may hold values from -64 to 64
- norm_gain: float32 [4096], replicated, may hold values from 0.25 to 1.75
- w_query: bfloat16 [4096, 2048], P('seq', 'dec'), may hold values from -0.140625 to 0.140625
- w_key: bfloat16 [4096, 512], P('seq', 'dec'), may hold values from -0.140625 to 0.140625
- w_value: bfloat16 [4096, 512], P('seq', 'dec'), may hold values from -0.09375 to 0.09375
- block_order: int32 [32], P('groups'), parts along dimension 0, may hold values from 0 to 15, as said below
- block_docs: int32 [32], P('groups'), parts along dimension 0, may hold values from 0 to 3, never falling along the last dimension, each value on 1 to 8 neighbouring positions
- head_owner: int32 [8], P('groups'), parts along dimension 0, may hold values from 0 to 3, as said below
- prev_kv: bfloat16 [2048, 2, 4, 128], P(('groups', 'seq', 'dec')), parts along dimension 0, may hold values from -6 to 6
Outputs:
- attended: bfloat16 [2048, 2048], P(('groups', 'seq'), 'dec'), parts along dimension 0
- decode_cache: bfloat16 [2048, 2, 4, 128], P(('groups', 'seq'), None, 'dec'), parts along dimension 0
The draws below stay inside these ranges and needn't reach their ends.
There are 2 independent parts, one for each index of `groups`. The reference program is written for one: setup_inputs(seed, part) draws one part's arguments, and reference() takes and returns one part's arrays. A program takes and returns all parts, laid end to end along the dimension named above; an argument that names none is the same for every part. Nothing has to cross between parts.
Inputs may be any that keep to these rules, and one draw needn't show every extreme that they name: `block_order`: cycle slots 2i and 2i + 1 hold the blocks b and 15 - b for some b; every block stands in exactly one slot. `head_owner`: each key-value head stands in exactly one decode slot.
All inputs are finite; a program needn't handle non-finite values.
Results may differ from the reference program's by a relative error of at most 0.0035.
The reference program's roundings to bfloat16 on the way (of `normed`, `values` and `probability`) count: a program that leaves them out, or rounds other values in their place, can miss the bound.
Values may be sent and summed in bfloat16 or wider, within the bound.
A program may use at most 64 MiB of HBM per device.

```python
import math
import jax
import jax.numpy as jnp
import numpy as np
from jax import lax

D = 4096
QH = 16
KVH = 4
HD = 128
TOKENS = 1024
BLK = 64
BLOCKS = 16
N_SEQ = 8


def query_base(key):
    return 3.0 * jax.random.truncated_normal(jax.random.fold_in(key, 11), -6.0, 6.0, (D, QH * HD), jnp.float32) / math.sqrt(D)


def draw_w_query(key, part):
    bound = 9.0 / math.sqrt(D)
    return jnp.clip(query_base(key), -bound, bound).astype(jnp.bfloat16)


def draw_w_key(key, part):
    bound = 9.0 / math.sqrt(D)
    fresh = jax.random.truncated_normal(jax.random.fold_in(key, 12), -6.0, 6.0, (D, KVH, HD), jnp.float32) / math.sqrt(D)
    return jnp.clip(fresh.reshape(D, KVH * HD), -bound, bound).astype(jnp.bfloat16)


def draw_tokens(key, part):
    base = jax.random.truncated_normal(jax.random.fold_in(key, 31), -6.0, 6.0, (TOKENS, D), jnp.float32)
    return base.astype(jnp.bfloat16)


def draw_block_order(key, part):
    pairs = BLOCKS // 2
    owner = jax.random.permutation(jax.random.fold_in(key, 21), pairs)
    flipped = jax.random.randint(jax.random.fold_in(key, 22), (pairs,), 0, 2)
    lower_block = owner
    upper_block = BLOCKS - 1 - owner
    leading = jnp.where(flipped == 1, upper_block, lower_block)
    trailing = jnp.where(flipped == 1, lower_block, upper_block)
    return jnp.stack([leading, trailing], 1).reshape(BLOCKS).astype(jnp.int32)


def draw_head_owner(key, part):
    return jax.random.permutation(jax.random.fold_in(key, 41), KVH).astype(jnp.int32)


def block_scale(rng, extent, pieces, smallest, high):
    level = 1.0
    for dim, blocks in pieces:
        draws = jax.random.uniform(jax.random.fold_in(jax.random.fold_in(rng, 6), dim), (blocks,), jnp.float32, smallest / len(pieces), high / len(pieces))
        level = level * jnp.repeat(jnp.exp(draws), extent[dim] // blocks).reshape((-1,) + (1,) * (len(extent) - 1 - dim))
    return level


def length_profile(number_of, total, limit, lean):
    loads = [(1 << 20) // math.isqrt(grade ** lean) + 1 for grade in range(2, number_of + 1)]
    surplus, given = total - limit - (number_of - 1), [1] * (number_of - 1)
    while surplus > 0:
        movable = [i for i in range(number_of - 1) if given[i] < limit]
        pool, budget = sum([loads[i] for i in movable]), surplus
        for i in movable:
            extra = min(limit - given[i], max(1, budget * loads[i] // pool), surplus)
            given[i] = given[i] + extra
            surplus = surplus - extra
    return np.array([limit] + given)


def ragged_sizes(own_key, number_of, total, most, slope):
    if number_of == 2:
        one = jax.random.randint(own_key, (), max(1, total - most), min(most, total - 1) + 1)
        return jnp.stack([one, total - one])
    sizes = jnp.asarray(length_profile(number_of, total, most, slope), jnp.int32)
    couples = (number_of - 1) // 2
    source_of, sink = sizes[1:1 + 2 * couples:2], sizes[2:2 + 2 * couples:2]
    slack = jnp.minimum(source_of - 1, most - sink)
    moved = jax.random.randint(jax.random.fold_in(own_key, 1), (couples,), 0, 1 << 20) % (slack + 1)
    sizes = sizes.at[1:1 + 2 * couples:2].set(source_of - moved).at[2:2 + 2 * couples:2].set(sink + moved)
    return sizes[jax.random.permutation(jax.random.fold_in(own_key, 2), number_of)]


def bell_draw(key, extent, width, limit, shards=(), kind=jnp.bfloat16):
    values = width * jax.random.normal(key, extent, jnp.float32)
    if shards:
        values = values * block_scale(key, extent, shards, -0.22, 0.18)
    return jnp.clip(values, -limit, limit).astype(kind)


def setup_inputs(seed: int = 0, part: int = 0) -> dict:
    key_list = jax.random.split(jax.random.key(seed), 10)
    part_keys = jax.random.split(jax.random.fold_in(key_list[9], part), 10)
    tokens = draw_tokens(jax.random.fold_in(jax.random.fold_in(key_list[9], part), 71), part)
    norm_gain = jnp.clip(1.0 + 0.15 * jax.random.normal(key_list[1], (D,), jnp.float32), 0.25, 1.75)
    w_query = draw_w_query(jax.random.fold_in(key_list[9], 71), part)
    w_key = draw_w_key(jax.random.fold_in(key_list[9], 71), part)
    w_value = bell_draw(key_list[4], (D, KVH * HD), D ** -0.5, 0.09375, ((0, 8), (1, 2)))
    block_order = draw_block_order(jax.random.fold_in(jax.random.fold_in(key_list[9], part), 71), part)
    block_docs = jnp.searchsorted(jnp.cumsum(ragged_sizes(part_keys[6], N_SEQ // 2, BLOCKS, N_SEQ, 2)), jnp.arange(BLOCKS), side="right").astype(jnp.int32)
    head_owner = draw_head_owner(jax.random.fold_in(jax.random.fold_in(key_list[9], part), 71), part)
    prev_kv = bell_draw(part_keys[8], (TOKENS, 2, KVH, HD), 1.0, 6.0, ((0, 16),))
    return dict(tokens=tokens, norm_gain=norm_gain, w_query=w_query, w_key=w_key, w_value=w_value, block_order=block_order, block_docs=block_docs, head_owner=head_owner, prev_kv=prev_kv)


def rotate(values, positions):
    half_width = values.shape[-1] // 2
    frequency = 500000.0 ** (-jnp.arange(half_width, dtype=jnp.float32) / half_width)
    angles = positions[:, None].astype(jnp.float32) * frequency[None, :]
    cosines = jnp.cos(angles)[:, None, :]
    sine_terms = jnp.sin(angles)[:, None, :]
    lower_half = values[..., :half_width]
    upper_half = values[..., half_width:]
    return jnp.concatenate([lower_half * cosines - upper_half * sine_terms, upper_half * cosines + lower_half * sine_terms], -1)

def reference(tokens, norm_gain, w_query, w_key, w_value, block_order, block_docs, head_owner, prev_kv):
    inputs = tokens.astype(jnp.float32)
    normed = (inputs * lax.rsqrt(lax.optimization_barrier(jnp.mean(inputs * inputs, -1, keepdims=True)) + 1e-05) * norm_gain).astype(jnp.bfloat16)
    row_ids = jnp.arange(TOKENS, dtype=jnp.int32)
    natural = block_order[row_ids // BLK]
    positions = natural * BLK + row_ids % BLK
    documents = block_docs[natural]
    queries = rotate(jnp.dot(normed, w_query, preferred_element_type=jnp.float32).reshape(TOKENS, QH, HD), positions).astype(jnp.bfloat16)
    key_rows = rotate(jnp.dot(normed, w_key, preferred_element_type=jnp.float32).reshape(TOKENS, KVH, HD), positions).astype(jnp.bfloat16)
    value_rows = jnp.dot(normed, w_value, preferred_element_type=jnp.float32).astype(jnp.bfloat16).reshape(TOKENS, KVH, HD)
    allowed = (positions[None, :] <= positions[:, None]) & (documents[None, :] == documents[:, None])
    group_size = QH // KVH
    scale = 1.0 / math.sqrt(HD)

    def one_head(head_index):
        query_head = queries[:, head_index]
        key_head = key_rows[:, head_index // group_size]
        value_head = value_rows[:, head_index // group_size]
        scores = jnp.dot(query_head, key_head.T, preferred_element_type=jnp.float32) * scale
        scores = jnp.where(allowed, scores, -jnp.inf)
        row_max = lax.optimization_barrier(jnp.max(scores, -1, keepdims=True))
        exponent_terms = jnp.exp(scores - row_max)
        running_sum = lax.optimization_barrier(jnp.sum(exponent_terms, -1, keepdims=True))
        probability = exponent_terms.astype(jnp.bfloat16)
        return jnp.dot(probability, value_head, preferred_element_type=jnp.float32) / running_sum
    heads_out = lax.map(one_head, jnp.arange(QH, dtype=jnp.int32))
    attended = jnp.transpose(heads_out, (1, 0, 2)).reshape(TOKENS, QH * HD).astype(jnp.bfloat16)
    decode_cache = prev_kv[:, :, head_owner, :]
    return (attended, decode_cache)
```

```python
import functools
import math

import jax
import jax.numpy as jnp
from jax import lax
from jax.experimental import pallas as pl
from jax.experimental.pallas import tpu as pltpu
from jax.sharding import PartitionSpec as P

HD = 128


def rotate(values, positions):
    half_width = values.shape[-1] // 2
    frequency = 500000.0 ** (-jnp.arange(half_width, dtype=jnp.float32) / half_width)
    angles = positions[:, None].astype(jnp.float32) * frequency[None, :]
    cosines = jnp.cos(angles)[:, None, :]
    sine_terms = jnp.sin(angles)[:, None, :]
    lower_half = values[..., :half_width]
    upper_half = values[..., half_width:]
    return jnp.concatenate(
        [
            lower_half * cosines - upper_half * sine_terms,
            upper_half * cosines + lower_half * sine_terms,
        ],
        -1,
    )


def general_plan(
    tokens, norm_gain, w_query, w_key, w_value, block_order, block_docs, head_owner, prev_kv
):
    rows_dev = tokens.shape[0]
    block_rows = rows_dev // 2
    inputs = tokens.astype(jnp.float32)
    normed = (
        inputs * lax.rsqrt(jnp.mean(inputs * inputs, -1, keepdims=True) + 1e-05) * norm_gain
    ).astype(jnp.bfloat16)

    def add_piece(piece):
        return jnp.dot(normed, piece, preferred_element_type=jnp.float32)

    pieces = (
        lax.all_gather(w_query, "seq", axis=0, tiled=True),
        lax.all_gather(w_key, "seq", axis=0, tiled=True),
        lax.all_gather(w_value, "seq", axis=0, tiled=True),
    )
    query_full, key_full, value_full = tuple((add_piece(piece) for piece in pieces))
    total_rows = rows_dev * lax.axis_size("seq")
    row_ids = jnp.arange(total_rows, dtype=jnp.int32)
    natural = jnp.take(block_order, row_ids // block_rows)
    pos_all = natural * block_rows + row_ids % block_rows
    doc_all = jnp.take(block_docs, natural)
    offset = lax.axis_index("seq") * rows_dev
    my_pos = lax.dynamic_slice_in_dim(pos_all, offset, rows_dev)
    my_doc = lax.dynamic_slice_in_dim(doc_all, offset, rows_dev)
    local_kv = key_full.shape[1] // HD
    local_heads = query_full.shape[1] // HD
    group_size = local_heads // local_kv
    queries = rotate(query_full.reshape(rows_dev, local_heads, HD), my_pos).astype(jnp.bfloat16)
    query_groups = queries.reshape(rows_dev, local_kv, group_size, HD).transpose(1, 2, 0, 3)
    key_rows = (
        rotate(key_full.reshape(rows_dev, local_kv, HD), my_pos)
        .astype(jnp.bfloat16)
        .reshape(rows_dev, local_kv * HD)
    )
    value_rows = value_full.astype(jnp.bfloat16)
    scale = 1.0 / math.sqrt(HD)
    start_max = jnp.full((local_kv, group_size, rows_dev, 1), -jnp.inf, jnp.float32)
    start_sum = jnp.zeros((local_kv, group_size, rows_dev, 1), jnp.float32)
    start_weighted = jnp.zeros((local_kv, group_size, rows_dev, HD), jnp.float32)
    key_piece = lax.all_gather(key_rows, "seq", axis=0, tiled=True)
    value_piece = lax.all_gather(value_rows, "seq", axis=0, tiled=True)
    count = key_piece.shape[0]
    allowed = (pos_all[None, :] <= my_pos[:, None]) & (doc_all[None, :] == my_doc[:, None])

    def update(state):
        running_max, running_sum, weighted = state
        scores = (
            jnp.einsum(
                "ghtd,sgd->ghts",
                query_groups,
                key_piece.reshape(count, local_kv, HD),
                preferred_element_type=jnp.float32,
            )
            * scale
        )
        scores = jnp.where(allowed, scores, -jnp.inf)
        new_max = jnp.max(scores, -1, keepdims=True)
        shift_by = jnp.where(new_max == -jnp.inf, 0.0, new_max)
        weights = jnp.exp(scores - shift_by)
        rescale = jnp.exp(running_max - shift_by)
        running_sum = running_sum * rescale + jnp.sum(weights, -1, keepdims=True)
        weighted = weighted * rescale + jnp.einsum(
            "ghts,sgd->ghtd",
            weights.astype(jnp.bfloat16),
            value_piece.reshape(count, local_kv, HD),
            preferred_element_type=jnp.float32,
        )
        return (new_max, running_sum, weighted)

    final_max, final_sum, final_weighted = lax.cond(
        jnp.any(allowed), update, lambda state: state, (start_max, start_sum, start_weighted)
    )
    attended = (
        (final_weighted / final_sum)
        .transpose(2, 0, 1, 3)
        .reshape(rows_dev, local_heads * HD)
        .astype(jnp.bfloat16)
    )
    head_count = prev_kv.shape[2]
    selector = (head_owner[:, None] == jnp.arange(head_count, dtype=jnp.int32)[None, :]).astype(
        jnp.bfloat16
    )
    ordered = jnp.einsum(
        "tcjd,sj->tcsd", prev_kv, selector, preferred_element_type=jnp.float32
    ).astype(jnp.bfloat16)
    decode_cache = lax.all_to_all(ordered, "dec", split_axis=2, concat_axis=0, tiled=True)
    return (attended, decode_cache)


def attend_kernel(
    sizes,
    order_ref,
    docs_ref,
    freq_ref,
    gain_ref,
    tok_in,
    wq_in,
    wk_in,
    wv_in,
    prev_in,
    out_ref,
    prev_out,
    tok,
    wbuf,
    normed,
    qbuf,
    kvbuf,
    csbuf,
    att,
    local_sem,
    home_send,
    homeq_recv,
    homekv_recv,
    rel_send,
    rel_recv,
    own_send,
    fwd_send,
    tok_recv,
    sib_send,
    sib_recv,
    prev_sem,
    kv_send,
    kv_recv,
    att_send,
    att_recv,
):
    X, A, Y, rows, R, hpg, slots, blk, T = sizes
    Rp = R // X
    half = rows // 2
    QW = hpg * HD
    x = lax.axis_index("groups")
    q = lax.axis_index("seq")
    d = lax.axis_index("dec")
    a = q // Y
    y = q % Y
    unit = a % 2

    def dev(x_, a_, y_, d_=None):
        return {"groups": x_, "seq": a_ * Y + y_, "dec": d if d_ is None else d_}

    def remote(src, dst, ssem, rsem, device):
        return pltpu.make_async_remote_copy(
            src_ref=src,
            dst_ref=dst,
            send_sem=ssem,
            recv_sem=rsem,
            device_id=device,
            device_id_type=pl.DeviceIdType.MESH,
        )

    sibling = dev(x, a, y, 1 - d)
    barrier = pltpu.get_barrier_semaphore()
    plane = [(i, j) for i in range(X) for j in range(Y) if (i, j) != (0, 0)]
    peers = [dev((x + i) % X, a, (y + j) % Y) for i, j in plane]
    peers += [dev(x, (a + t) % A, y) for t in range(1, A)]
    mate = a + 1 - 2 * unit
    peers += [dev(x, mate, (y + j) % Y) for j in range(1, Y)]
    peers.append(sibling)
    for peer in peers:
        pl.semaphore_signal(barrier, inc=1, device_id=peer, device_id_type=pl.DeviceIdType.MESH)
    pl.semaphore_wait(barrier, len(peers))

    def w_rows(a_, y_, x_):
        return pl.ds(pl.multiple_of((a_ * Y + y_) * R + x_ * Rp, Rp), Rp)

    part = pl.ds(pl.multiple_of(x * Rp, Rp), Rp)

    def kv_source(t):
        return wv_in if t % 2 else wk_in

    def home_copies(t):
        kv_cols = pl.ds((t // 2) * HD, HD)
        return (
            remote(
                wq_in.at[part, pl.ds(t * QW, QW)],
                wbuf.at[w_rows(a, y, x), pl.ds(0, QW)],
                home_send.at[0, t],
                homeq_recv.at[a],
                dev(x, t, y),
            ),
            remote(
                kv_source(t).at[part, kv_cols],
                wbuf.at[w_rows(a, y, x), pl.ds(QW, HD)],
                home_send.at[1, t],
                homekv_recv.at[a],
                dev(x, t, y),
            ),
        )

    def local_copies(t):
        rows_all = pl.ds(pl.multiple_of(q * R, R), R)
        return (
            pltpu.make_async_copy(
                wq_in.at[:, pl.ds(t * QW, QW)],
                wbuf.at[rows_all, pl.ds(0, QW)],
                local_sem.at[0],
            ),
            pltpu.make_async_copy(
                kv_source(t).at[:, pl.ds((t // 2) * HD, HD)],
                wbuf.at[rows_all, pl.ds(QW, HD)],
                local_sem.at[1],
            ),
        )

    for t in range(A):

        @pl.when(a == t)
        def _():
            for copy in local_copies(t):
                copy.start()

        @pl.when(a != t)
        def _():
            for copy in home_copies(t):
                copy.start()

    my_half = pl.ds(pl.multiple_of(d * half, half), half)
    other_half = pl.ds(pl.multiple_of((1 - d) * half, half), half)

    def own_push(side):
        return remote(
            tok_in.at[my_half],
            tok.at[a, my_half],
            own_send.at[side],
            tok_recv.at[a],
            dev(x, a + 1 - 2 * side, y),
        )

    @pl.when(a + 1 < A)
    def _():
        own_push(0).start()

    @pl.when(a >= 1)
    def _():
        own_push(1).start()

    own_tok = pltpu.make_async_copy(tok_in, tok.at[a], local_sem.at[2])
    own_tok.start()
    prev_copy = remote(prev_in, prev_out, prev_sem.at[0], prev_sem.at[1], sibling)
    prev_copy.start()

    def relay(t, index, i, j):
        src = wbuf.at[w_rows(t, y, x)]
        return remote(
            src,
            src,
            rel_send.at[t, index],
            rel_recv.at[t, y, x],
            dev((x + i) % X, a, (y + j) % Y),
        )

    for t in range(A):

        @pl.when(a == t)
        def _():
            for copy in local_copies(t):
                copy.wait()
            for index, (i, j) in enumerate(plane):
                if j:
                    relay(t, index, i, j).start()

    lane = lax.broadcasted_iota(jnp.int32, (rows, HD), 1)
    row_id = lax.broadcasted_iota(jnp.int32, (rows, 1), 0)

    def row_values(c, table):
        value = jnp.zeros((rows, 1), jnp.int32)
        for i in range(slots):
            entry = table(order_ref[(c * Y + y) * slots + i])
            value = jnp.where(row_id // blk == i, entry, value)
        return value

    def row_positions(c):
        return row_values(c, lambda n: n) * blk + row_id % blk

    def angles(c, carry):
        angle = row_positions(c).astype(jnp.float32) * freq_ref[...]
        csbuf[0, c] = jnp.cos(angle)
        sine = jnp.sin(angle)
        csbuf[1, c] = jnp.where(lane < HD // 2, -sine, sine)
        return carry

    lax.fori_loop(0, A, angles, 0)

    for o in range(1, A):
        t = (a + o) % A
        src = wbuf.at[w_rows(t, y, x)]
        remote(
            wq_in.at[part, pl.ds(0, QW)],
            wbuf.at[w_rows(t, y, x), pl.ds(0, QW)],
            home_send.at[0, 0],
            homeq_recv.at[t],
            sibling,
        ).wait_recv()
        remote(
            wk_in.at[part, pl.ds(0, HD)],
            wbuf.at[w_rows(t, y, x), pl.ds(QW, HD)],
            home_send.at[1, 0],
            homekv_recv.at[t],
            sibling,
        ).wait_recv()
        for index, (i, j) in enumerate(plane):
            relay(t, index, i, j).start()

    def forward(c, to):
        return remote(
            tok.at[c, my_half],
            tok.at[c, my_half],
            fwd_send.at[c],
            tok_recv.at[c],
            dev(x, to, y),
        )

    def share(c):
        return remote(
            tok.at[c, my_half], tok.at[c, my_half], sib_send.at[c], sib_recv.at[c], sibling
        )

    for s in range(1, A):

        @pl.when(a >= s)
        def _():
            c = a - s
            forward(c, a).wait_recv()

            @pl.when(a + 1 < A)
            def _():
                forward(c, a + 1).start()

            share(c).start()

        @pl.when(a + s < A)
        def _():
            c = a + s
            forward(c, a).wait_recv()

            @pl.when(a >= 1)
            def _():
                forward(c, a - 1).start()

            share(c).start()

    own_tok.wait()
    for o in range(A):
        t = (a + o) % A
        for i, j in plane:
            if o or j:
                src = wbuf.at[w_rows(t, (y + j) % Y, (x + i) % X)]
                remote(
                    src,
                    src,
                    rel_send.at[0, 0],
                    rel_recv.at[t, (y + j) % Y, (x + i) % X],
                    sibling,
                ).wait_recv()

    def pick(s):
        value, bit = 0, 1
        while bit < A:
            value = value + bit * ((a // bit + s // bit) % 2)
            bit *= 2
        return value

    def kv_peer(dy, da):
        return dev(x, a - unit + (unit + da) % 2, (y + dy) % Y)

    kv_plan = [(dy, da) for dy in range(Y) for da in range(2) if (dy, da) != (0, 0)]

    def kv_push(s, c, index, dy, da):
        src = kvbuf.at[unit, c * Y + y]
        return remote(src, src, kv_send.at[s, index], kv_recv.at[unit, c, y], kv_peer(dy, da))

    def project(s, carry):
        c = pick(s)

        @pl.when(s > 0)
        def _():
            remote(
                tok.at[c, other_half],
                tok.at[c, other_half],
                sib_send.at[c],
                sib_recv.at[c],
                sibling,
            ).wait_recv()

        inputs = tok[c].astype(jnp.float32)
        mean = jnp.mean(inputs * inputs, -1, keepdims=True)
        normed[...] = (inputs * lax.rsqrt(mean + 1e-05) * gain_ref[...]).astype(jnp.bfloat16)
        cosine = csbuf[0, c]
        sine = csbuf[1, c]
        product = jnp.dot(normed[...], wbuf[...], preferred_element_type=jnp.float32)

        def turn(v):
            return v * cosine + pltpu.roll(v, HD // 2, 1) * sine

        raw = product[:, QW:]
        kvbuf[unit, c * Y + y] = jnp.where(unit == 0, turn(raw), raw).astype(jnp.bfloat16)
        for h in range(hpg):
            qbuf[c, :, h * HD : (h + 1) * HD] = turn(product[:, h * HD : (h + 1) * HD]).astype(
                jnp.bfloat16
            )
        for index, (dy, da) in enumerate(kv_plan):
            kv_push(s, c, index, dy, da).start()
        return carry

    lax.fori_loop(0, A, project, 0)

    for s in range(A):
        c = pick(s)
        for dy, da in kv_plan:
            u = (unit + da) % 2
            dst = kvbuf.at[u, c * Y + (y + dy) % Y]
            remote(
                dst, dst, kv_send.at[0, 0], kv_recv.at[u, c, (y + dy) % Y], sibling
            ).wait_recv()

    key_id = lax.broadcasted_iota(jnp.int32, (1, T), 1)
    key_pos = jnp.zeros((1, T), jnp.int32)
    key_doc = jnp.zeros((1, T), jnp.int32)
    for i in range(T // blk):
        here = key_id // blk == i
        natural = order_ref[i]
        key_pos = jnp.where(here, natural * blk, key_pos)
        key_doc = jnp.where(here, docs_ref[natural], key_doc)
    key_pos = key_pos + key_id % blk
    scale = 1.0 / math.sqrt(HD)
    out_cols = pl.ds(pl.multiple_of(a * QW, QW), QW)

    def att_push(s, c):
        return remote(
            att.at[c], out_ref.at[:, out_cols], att_send.at[s], att_recv.at[a], dev(x, c, y)
        )

    def attend(s, carry):
        c = pick(A - 1 - s)
        allowed = (key_pos <= row_positions(c)) & (
            key_doc == row_values(c, lambda n: docs_ref[n])
        )
        keys = kvbuf[0].reshape(T, HD)
        values = kvbuf[1].reshape(T, HD)
        for h in range(hpg):
            scores = (
                lax.dot_general(
                    qbuf[c, :, h * HD : (h + 1) * HD],
                    keys,
                    (((1,), (1,)), ((), ())),
                    preferred_element_type=jnp.float32,
                )
                * scale
            )
            scores = jnp.where(allowed, scores, -jnp.inf)
            weights = jnp.exp(scores - jnp.max(scores, -1, keepdims=True))
            total = jnp.sum(weights, -1, keepdims=True)
            weighted = jnp.dot(
                weights.astype(jnp.bfloat16), values, preferred_element_type=jnp.float32
            )
            att[c, :, h * HD : (h + 1) * HD] = (weighted / total).astype(jnp.bfloat16)

        @pl.when(s < A - 1)
        def _():
            att_push(s, c).start()

        return carry

    lax.fori_loop(0, A, attend, 0)
    own_out = pltpu.make_async_copy(att.at[a], out_ref.at[:, out_cols], local_sem.at[3])
    own_out.start()

    for t in range(A):

        @pl.when(a != t)
        def _():
            for copy in home_copies(t):
                copy.wait_send()
            for index, (i, j) in enumerate(plane):
                relay(t, index, i, j).wait_send()

        @pl.when(a == t)
        def _():
            for index, (i, j) in enumerate(plane):
                if j:
                    relay(t, index, i, j).wait_send()

    @pl.when(a + 1 < A)
    def _():
        own_push(0).wait_send()

    @pl.when(a >= 1)
    def _():
        own_push(1).wait_send()

    for s in range(1, A):

        @pl.when(a >= s)
        def _():
            share(a - s).wait_send()

            @pl.when(a + 1 < A)
            def _():
                forward(a - s, a + 1).wait_send()

        @pl.when(a + s < A)
        def _():
            share(a + s).wait_send()

            @pl.when(a >= 1)
            def _():
                forward(a + s, a - 1).wait_send()

    for s in range(A):
        for index, (dy, da) in enumerate(kv_plan):
            kv_push(s, pick(s), index, dy, da).wait_send()
    prev_copy.wait()
    own_out.wait()
    for s in range(A - 1):
        att_push(s, pick(A - 1 - s)).wait_send()
    for o in range(1, A):
        t = (a + o) % A
        cols = pl.ds(pl.multiple_of(t * QW, QW), QW)
        remote(
            att.at[0], out_ref.at[:, cols], att_send.at[0], att_recv.at[t], sibling
        ).wait_recv()


def column_plan(
    X, tokens, norm_gain, w_query, w_key, w_value, block_order, block_docs, head_owner, prev_kv
):
    n_seq = lax.axis_size("seq")
    rows, width = tokens.shape
    R = w_query.shape[0]
    local_kv = w_key.shape[1] // HD
    local_heads = w_query.shape[1] // HD
    A = 2 * local_kv
    Y = n_seq // A
    hpg = local_heads // A
    slots = block_order.shape[0] // n_seq
    blk = rows // slots
    T = n_seq * rows
    QW = hpg * HD
    frequency = 500000.0 ** (-jnp.arange(HD // 2, dtype=jnp.float32) / (HD // 2))
    freq = jnp.concatenate([frequency, frequency])[None, :]
    sizes = (X, A, Y, rows, R, hpg, slots, blk, T)
    dma = pltpu.SemaphoreType.DMA
    smem = pl.BlockSpec(memory_space=pltpu.SMEM)
    vmem = pl.BlockSpec(memory_space=pltpu.VMEM)
    anywhere = pl.BlockSpec(memory_space=pl.ANY)
    attended, other = pl.pallas_call(
        functools.partial(attend_kernel, sizes),
        out_shape=(
            jax.ShapeDtypeStruct((rows, local_heads * HD), jnp.bfloat16),
            jax.ShapeDtypeStruct(prev_kv.shape, prev_kv.dtype),
        ),
        in_specs=[smem, smem, vmem, vmem] + [anywhere] * 5,
        out_specs=(vmem, anywhere),
        scratch_shapes=[
            pltpu.VMEM((A, rows, width), jnp.bfloat16),
            pltpu.VMEM((width, QW + HD), jnp.bfloat16),
            pltpu.VMEM((rows, width), jnp.bfloat16),
            pltpu.VMEM((A, rows, QW), jnp.bfloat16),
            pltpu.VMEM((2, n_seq, rows, HD), jnp.bfloat16),
            pltpu.VMEM((2, A, rows, HD), jnp.float32),
            pltpu.VMEM((A, rows, QW), jnp.bfloat16),
            dma((4,)),
            dma((2, A)),
            dma((A,)),
            dma((A,)),
            dma((A, X * Y)),
            dma((A, Y, X)),
            dma((2,)),
            dma((A,)),
            dma((A,)),
            dma((A,)),
            dma((A,)),
            dma((2,)),
            dma((A, 2 * Y)),
            dma((2, A, Y)),
            dma((A,)),
            dma((A,)),
        ],
        compiler_params=pltpu.CompilerParams(
            collective_id=0, has_side_effects=True, vmem_limit_bytes=48 * 1024 * 1024
        ),
    )(
        block_order,
        block_docs,
        freq,
        norm_gain[None, :],
        tokens,
        w_query,
        w_key,
        w_value,
        prev_kv,
    )
    d = lax.axis_index("dec")
    head_count = prev_kv.shape[2]
    mine = head_count // 2
    owner = lax.dynamic_slice_in_dim(head_owner, d * mine, mine)
    both = jnp.concatenate(
        [jnp.where(d == 0, prev_kv, other), jnp.where(d == 0, other, prev_kv)], 0
    )
    picks = []
    for s in range(mine):
        chosen = both[:, :, 0]
        for j in range(1, head_count):
            chosen = jnp.where(owner[s] == j, both[:, :, j], chosen)
        picks.append(chosen)
    return attended, jnp.stack(picks, 2)


def solution(mesh):
    in_specs = (
        P(("groups", "seq"), None),
        P(),
        P("seq", "dec"),
        P("seq", "dec"),
        P("seq", "dec"),
        P("groups"),
        P("groups"),
        P("groups"),
        P(("groups", "seq", "dec"), None, None, None),
    )
    out_specs = (P(("groups", "seq"), "dec"), P(("groups", "seq"), None, "dec", None))
    X = mesh.shape["groups"]
    n_seq = mesh.shape["seq"]

    def per_device(tokens, norm_gain, w_query, w_key, w_value, *rest):
        A = 2 * (w_key.shape[1] // HD)
        heads = w_query.shape[1] // HD
        fits = (
            mesh.shape["dec"] == 2
            and A & (A - 1) == 0
            and n_seq % A == 0
            and heads % A == 0
            and w_query.shape[0] % (16 * X) == 0
            and tokens.shape[0] % 32 == 0
        )
        plan = functools.partial(column_plan, X) if fits else general_plan
        return plan(tokens, norm_gain, w_query, w_key, w_value, *rest)

    return jax.shard_map(
        per_device, mesh=mesh, in_specs=in_specs, out_specs=out_specs, check_vma=False
    )
```

```python
import functools
import math

import jax
import jax.numpy as jnp
from jax import lax
from jax.experimental import pallas as pl
from jax.experimental.pallas import tpu as pltpu
from jax.sharding import PartitionSpec as P

HD = 128


def rotate(values, positions):
    half_width = values.shape[-1] // 2
    frequency = 500000.0 ** (-jnp.arange(half_width, dtype=jnp.float32) / half_width)
    angles = positions[:, None].astype(jnp.float32) * frequency[None, :]
    cosines = jnp.cos(angles)[:, None, :]
    sine_terms = jnp.sin(angles)[:, None, :]
    lower_half = values[..., :half_width]
    upper_half = values[..., half_width:]
    return jnp.concatenate(
        [
            lower_half * cosines - upper_half * sine_terms,
            upper_half * cosines + lower_half * sine_terms,
        ],
        -1,
    )


def general_plan(
    tokens, norm_gain, w_query, w_key, w_value, block_order, block_docs, head_owner, prev_kv
):
    rows_dev = tokens.shape[0]
    block_rows = rows_dev // 2
    inputs = tokens.astype(jnp.float32)
    normed = (
        inputs * lax.rsqrt(jnp.mean(inputs * inputs, -1, keepdims=True) + 1e-05) * norm_gain
    ).astype(jnp.bfloat16)

    def add_piece(piece):
        return jnp.dot(normed, piece, preferred_element_type=jnp.float32)

    pieces = (
        lax.all_gather(w_query, "seq", axis=0, tiled=True),
        lax.all_gather(w_key, "seq", axis=0, tiled=True),
        lax.all_gather(w_value, "seq", axis=0, tiled=True),
    )
    query_full, key_full, value_full = tuple((add_piece(piece) for piece in pieces))
    total_rows = rows_dev * lax.axis_size("seq")
    row_ids = jnp.arange(total_rows, dtype=jnp.int32)
    natural = jnp.take(block_order, row_ids // block_rows)
    pos_all = natural * block_rows + row_ids % block_rows
    doc_all = jnp.take(block_docs, natural)
    offset = lax.axis_index("seq") * rows_dev
    my_pos = lax.dynamic_slice_in_dim(pos_all, offset, rows_dev)
    my_doc = lax.dynamic_slice_in_dim(doc_all, offset, rows_dev)
    local_kv = key_full.shape[1] // HD
    local_heads = query_full.shape[1] // HD
    group_size = local_heads // local_kv
    queries = rotate(query_full.reshape(rows_dev, local_heads, HD), my_pos).astype(jnp.bfloat16)
    query_groups = queries.reshape(rows_dev, local_kv, group_size, HD).transpose(1, 2, 0, 3)
    key_rows = (
        rotate(key_full.reshape(rows_dev, local_kv, HD), my_pos)
        .astype(jnp.bfloat16)
        .reshape(rows_dev, local_kv * HD)
    )
    value_rows = value_full.astype(jnp.bfloat16)
    scale = 1.0 / math.sqrt(HD)
    start_max = jnp.full((local_kv, group_size, rows_dev, 1), -jnp.inf, jnp.float32)
    start_sum = jnp.zeros((local_kv, group_size, rows_dev, 1), jnp.float32)
    start_weighted = jnp.zeros((local_kv, group_size, rows_dev, HD), jnp.float32)
    key_piece = lax.all_gather(key_rows, "seq", axis=0, tiled=True)
    value_piece = lax.all_gather(value_rows, "seq", axis=0, tiled=True)
    count = key_piece.shape[0]
    allowed = (pos_all[None, :] <= my_pos[:, None]) & (doc_all[None, :] == my_doc[:, None])

    def update(state):
        running_max, running_sum, weighted = state
        scores = (
            jnp.einsum(
                "ghtd,sgd->ghts",
                query_groups,
                key_piece.reshape(count, local_kv, HD),
                preferred_element_type=jnp.float32,
            )
            * scale
        )
        scores = jnp.where(allowed, scores, -jnp.inf)
        new_max = jnp.max(scores, -1, keepdims=True)
        shift_by = jnp.where(new_max == -jnp.inf, 0.0, new_max)
        weights = jnp.exp(scores - shift_by)
        rescale = jnp.exp(running_max - shift_by)
        running_sum = running_sum * rescale + jnp.sum(weights, -1, keepdims=True)
        weighted = weighted * rescale + jnp.einsum(
            "ghts,sgd->ghtd",
            weights.astype(jnp.bfloat16),
            value_piece.reshape(count, local_kv, HD),
            preferred_element_type=jnp.float32,
        )
        return (new_max, running_sum, weighted)

    final_max, final_sum, final_weighted = lax.cond(
        jnp.any(allowed), update, lambda state: state, (start_max, start_sum, start_weighted)
    )
    attended = (
        (final_weighted / final_sum)
        .transpose(2, 0, 1, 3)
        .reshape(rows_dev, local_heads * HD)
        .astype(jnp.bfloat16)
    )
    head_count = prev_kv.shape[2]
    selector = (head_owner[:, None] == jnp.arange(head_count, dtype=jnp.int32)[None, :]).astype(
        jnp.bfloat16
    )
    ordered = jnp.einsum(
        "tcjd,sj->tcsd", prev_kv, selector, preferred_element_type=jnp.float32
    ).astype(jnp.bfloat16)
    decode_cache = lax.all_to_all(ordered, "dec", split_axis=2, concat_axis=0, tiled=True)
    return (attended, decode_cache)


def attend_kernel(
    sizes,
    order_ref,
    docs_ref,
    freq_ref,
    gain_ref,
    tok_in,
    wq_in,
    wk_in,
    wv_in,
    prev_in,
    out_ref,
    prev_out,
    tok,
    wbuf,
    normed,
    qbuf,
    kvbuf,
    csbuf,
    att,
    local_sem,
    home_send,
    homeq_recv,
    homekv_recv,
    rel_send,
    rel_recv,
    own_send,
    fwd_send,
    tok_recv,
    sib_send,
    sib_recv,
    prev_sem,
    kv_send,
    kv_recv,
    att_send,
    att_recv,
):
    X, A, Y, rows, R, hpg, slots, blk, T = sizes
    Rp = R // X
    half = rows // 2
    QW = hpg * HD
    x = lax.axis_index("groups")
    q = lax.axis_index("seq")
    d = lax.axis_index("dec")
    a = q // Y
    y = q % Y
    unit = a % 2

    def dev(x_, a_, y_, d_=None):
        return {"groups": x_, "seq": a_ * Y + y_, "dec": d if d_ is None else d_}

    def remote(src, dst, ssem, rsem, device):
        return pltpu.make_async_remote_copy(
            src_ref=src,
            dst_ref=dst,
            send_sem=ssem,
            recv_sem=rsem,
            device_id=device,
            device_id_type=pl.DeviceIdType.MESH,
        )

    sibling = dev(x, a, y, 1 - d)
    barrier = pltpu.get_barrier_semaphore()
    plane = [(i, j) for i in range(X) for j in range(Y) if (i, j) != (0, 0)]
    peers = [dev((x + i) % X, a, (y + j) % Y) for i, j in plane]
    peers += [dev(x, (a + t) % A, y) for t in range(1, A)]
    mate = a + 1 - 2 * unit
    peers += [dev(x, mate, (y + j) % Y) for j in range(1, Y)]
    peers.append(sibling)
    for peer in peers:
        pl.semaphore_signal(barrier, inc=1, device_id=peer, device_id_type=pl.DeviceIdType.MESH)
    pl.semaphore_wait(barrier, len(peers))

    def w_rows(a_, y_, x_):
        return pl.ds(pl.multiple_of((a_ * Y + y_) * R + x_ * Rp, Rp), Rp)

    part = pl.ds(pl.multiple_of(x * Rp, Rp), Rp)

    def kv_source(t):
        return wv_in if t % 2 else wk_in

    def home_copies(t):
        kv_cols = pl.ds((t // 2) * HD, HD)
        return (
            remote(
                wq_in.at[part, pl.ds(t * QW, QW)],
                wbuf.at[w_rows(a, y, x), pl.ds(0, QW)],
                home_send.at[0, t],
                homeq_recv.at[a],
                dev(x, t, y),
            ),
            remote(
                kv_source(t).at[part, kv_cols],
                wbuf.at[w_rows(a, y, x), pl.ds(QW, HD)],
                home_send.at[1, t],
                homekv_recv.at[a],
                dev(x, t, y),
            ),
        )

    def local_copies(t):
        rows_all = pl.ds(pl.multiple_of(q * R, R), R)
        return (
            pltpu.make_async_copy(
                wq_in.at[:, pl.ds(t * QW, QW)],
                wbuf.at[rows_all, pl.ds(0, QW)],
                local_sem.at[0],
            ),
            pltpu.make_async_copy(
                kv_source(t).at[:, pl.ds((t // 2) * HD, HD)],
                wbuf.at[rows_all, pl.ds(QW, HD)],
                local_sem.at[1],
            ),
        )

    for t in range(A):

        @pl.when(a == t)
        def _():
            for copy in local_copies(t):
                copy.start()

        @pl.when(a != t)
        def _():
            for copy in home_copies(t):
                copy.start()

    my_half = pl.ds(pl.multiple_of(d * half, half), half)
    other_half = pl.ds(pl.multiple_of((1 - d) * half, half), half)

    def own_push(side):
        return remote(
            tok_in.at[my_half],
            tok.at[a, my_half],
            own_send.at[side],
            tok_recv.at[a],
            dev(x, a + 1 - 2 * side, y),
        )

    @pl.when(a + 1 < A)
    def _():
        own_push(0).start()

    @pl.when(a >= 1)
    def _():
        own_push(1).start()

    own_tok = pltpu.make_async_copy(tok_in, tok.at[a], local_sem.at[2])
    own_tok.start()
    prev_copy = remote(prev_in, prev_out, prev_sem.at[0], prev_sem.at[1], sibling)
    prev_copy.start()

    def relay(t, index, i, j):
        src = wbuf.at[w_rows(t, y, x)]
        return remote(
            src,
            src,
            rel_send.at[t, index],
            rel_recv.at[t, y, x],
            dev((x + i) % X, a, (y + j) % Y),
        )

    for t in range(A):

        @pl.when(a == t)
        def _():
            for copy in local_copies(t):
                copy.wait()
            for index, (i, j) in enumerate(plane):
                if j:
                    relay(t, index, i, j).start()

    lane = lax.broadcasted_iota(jnp.int32, (rows, HD), 1)
    row_id = lax.broadcasted_iota(jnp.int32, (rows, 1), 0)

    def row_values(c, table):
        value = jnp.zeros((rows, 1), jnp.int32)
        for i in range(slots):
            entry = table(order_ref[(c * Y + y) * slots + i])
            value = jnp.where(row_id // blk == i, entry, value)
        return value

    def row_positions(c):
        return row_values(c, lambda n: n) * blk + row_id % blk

    def angles(c, carry):
        angle = row_positions(c).astype(jnp.float32) * freq_ref[...]
        csbuf[0, c] = jnp.cos(angle)
        sine = jnp.sin(angle)
        csbuf[1, c] = jnp.where(lane < HD // 2, -sine, sine)
        return carry

    lax.fori_loop(0, A, angles, 0)

    for o in range(1, A):
        t = (a + o) % A
        src = wbuf.at[w_rows(t, y, x)]
        remote(
            wq_in.at[part, pl.ds(0, QW)],
            wbuf.at[w_rows(t, y, x), pl.ds(0, QW)],
            home_send.at[0, 0],
            homeq_recv.at[t],
            sibling,
        ).wait_recv()
        remote(
            wk_in.at[part, pl.ds(0, HD)],
            wbuf.at[w_rows(t, y, x), pl.ds(QW, HD)],
            home_send.at[1, 0],
            homekv_recv.at[t],
            sibling,
        ).wait_recv()
        for index, (i, j) in enumerate(plane):
            relay(t, index, i, j).start()

    def forward(c, to):
        return remote(
            tok.at[c, my_half],
            tok.at[c, my_half],
            fwd_send.at[c],
            tok_recv.at[c],
            dev(x, to, y),
        )

    def share(c):
        return remote(
            tok.at[c, my_half], tok.at[c, my_half], sib_send.at[c], sib_recv.at[c], sibling
        )

    def token_step(s):
        @pl.when(a >= s)
        def _():
            c = a - s
            forward(c, a).wait_recv()

            @pl.when(a + 1 < A)
            def _():
                forward(c, a + 1).start()

            share(c).start()

        @pl.when(a + s < A)
        def _():
            c = a + s
            forward(c, a).wait_recv()

            @pl.when(a >= 1)
            def _():
                forward(c, a - 1).start()

            share(c).start()

    def pick(s):
        value, bit = 0, 1
        while bit < A:
            value = value + bit * ((a // bit + s // bit) % 2)
            bit *= 2
        return value

    def kv_peer(dy, da):
        return dev(x, a - unit + (unit + da) % 2, (y + dy) % Y)

    kv_plan = [(dy, da) for dy in range(Y) for da in range(2) if (dy, da) != (0, 0)]

    def kv_push(s, c, index, dy, da):
        src = kvbuf.at[unit, c * Y + y]
        return remote(src, src, kv_send.at[s, index], kv_recv.at[unit, c, y], kv_peer(dy, da))

    def normalize(s):
        c = pick(s)
        if s == 0:
            own_tok.wait()
        else:
            other = tok.at[c, other_half]
            remote(other, other, sib_send.at[c], sib_recv.at[c], sibling).wait_recv()

        def block(i, carry):
            span = pl.ds(pl.multiple_of(i * 16, 16), 16)
            inputs = tok[c, span].astype(jnp.float32)
            mean = jnp.mean(inputs * inputs, -1, keepdims=True)
            normed[c, span] = (inputs * lax.rsqrt(mean + 1e-05) * gain_ref[...]).astype(
                jnp.bfloat16
            )
            return carry

        lax.fori_loop(0, rows // 16, block, 0, unroll=2)

    def project(s, carry):
        c = pick(s)
        cosine = csbuf[0, c]
        sine = csbuf[1, c]

        def turn(v):
            return v * cosine + pltpu.roll(v, HD // 2, 1) * sine

        raw = jnp.dot(normed[c], wbuf[:, QW:], preferred_element_type=jnp.float32)
        kvbuf[unit, c * Y + y] = jnp.where(unit == 0, turn(raw), raw).astype(jnp.bfloat16)
        product = jnp.dot(normed[c], wbuf[:, :QW], preferred_element_type=jnp.float32)
        for index, (dy, da) in enumerate(kv_plan):
            kv_push(s, c, index, dy, da).start()
        for h in range(hpg):
            qbuf[c, :, h * HD : (h + 1) * HD] = turn(product[:, h * HD : (h + 1) * HD]).astype(
                jnp.bfloat16
            )
        return carry

    normalize(0)
    for s in range(1, A - 1):
        token_step(s)
        normalize(s)
    for o in range(A):
        t = (a + o) % A
        for i, j in plane:
            if o or j:
                src = wbuf.at[w_rows(t, (y + j) % Y, (x + i) % X)]
                remote(
                    src,
                    src,
                    rel_send.at[0, 0],
                    rel_recv.at[t, (y + j) % Y, (x + i) % X],
                    sibling,
                ).wait_recv()

    lax.fori_loop(0, A - 1, project, 0)
    token_step(A - 1)
    normalize(A - 1)
    project(A - 1, 0)

    for s in range(A):
        c = pick(s)
        for dy, da in kv_plan:
            u = (unit + da) % 2
            dst = kvbuf.at[u, c * Y + (y + dy) % Y]
            remote(
                dst, dst, kv_send.at[0, 0], kv_recv.at[u, c, (y + dy) % Y], sibling
            ).wait_recv()

    key_id = lax.broadcasted_iota(jnp.int32, (1, T), 1)
    key_pos = jnp.zeros((1, T), jnp.int32)
    key_doc = jnp.zeros((1, T), jnp.int32)
    for i in range(T // blk):
        here = key_id // blk == i
        natural = order_ref[i]
        key_pos = jnp.where(here, natural * blk, key_pos)
        key_doc = jnp.where(here, docs_ref[natural], key_doc)
    key_pos = key_pos + key_id % blk
    scale = 1.0 / math.sqrt(HD)
    out_cols = pl.ds(pl.multiple_of(a * QW, QW), QW)

    def att_push(s, c):
        return remote(
            att.at[c], out_ref.at[:, out_cols], att_send.at[s], att_recv.at[a], dev(x, c, y)
        )

    def attend(s, carry):
        c = pick(A - 1 - s)
        allowed = (key_pos <= row_positions(c)) & (
            key_doc == row_values(c, lambda n: docs_ref[n])
        )
        keys = kvbuf[0].reshape(T, HD)
        values = kvbuf[1].reshape(T, HD)
        for h in range(hpg):
            scores = (
                lax.dot_general(
                    qbuf[c, :, h * HD : (h + 1) * HD],
                    keys,
                    (((1,), (1,)), ((), ())),
                    preferred_element_type=jnp.float32,
                )
                * scale
            )
            scores = jnp.where(allowed, scores, -jnp.inf)
            weights = jnp.exp(scores - jnp.max(scores, -1, keepdims=True))
            total = jnp.sum(weights, -1, keepdims=True)
            weighted = jnp.dot(
                weights.astype(jnp.bfloat16), values, preferred_element_type=jnp.float32
            )
            att[c, :, h * HD : (h + 1) * HD] = (weighted / total).astype(jnp.bfloat16)

        @pl.when(s < A - 1)
        def _():
            att_push(s, c).start()

        return carry

    lax.fori_loop(0, A, attend, 0)
    own_out = pltpu.make_async_copy(att.at[a], out_ref.at[:, out_cols], local_sem.at[3])
    own_out.start()

    for t in range(A):

        @pl.when(a != t)
        def _():
            for copy in home_copies(t):
                copy.wait_send()
            for index, (i, j) in enumerate(plane):
                relay(t, index, i, j).wait_send()

        @pl.when(a == t)
        def _():
            for index, (i, j) in enumerate(plane):
                if j:
                    relay(t, index, i, j).wait_send()

    @pl.when(a + 1 < A)
    def _():
        own_push(0).wait_send()

    @pl.when(a >= 1)
    def _():
        own_push(1).wait_send()

    for s in range(1, A):

        @pl.when(a >= s)
        def _():
            share(a - s).wait_send()

            @pl.when(a + 1 < A)
            def _():
                forward(a - s, a + 1).wait_send()

        @pl.when(a + s < A)
        def _():
            share(a + s).wait_send()

            @pl.when(a >= 1)
            def _():
                forward(a + s, a - 1).wait_send()

    for s in range(A):
        for index, (dy, da) in enumerate(kv_plan):
            kv_push(s, pick(s), index, dy, da).wait_send()
    prev_copy.wait()
    own_out.wait()
    for s in range(A - 1):
        att_push(s, pick(A - 1 - s)).wait_send()
    for o in range(1, A):
        t = (a + o) % A
        cols = pl.ds(pl.multiple_of(t * QW, QW), QW)
        remote(
            att.at[0], out_ref.at[:, cols], att_send.at[0], att_recv.at[t], sibling
        ).wait_recv()


def column_plan(
    X, tokens, norm_gain, w_query, w_key, w_value, block_order, block_docs, head_owner, prev_kv
):
    n_seq = lax.axis_size("seq")
    rows, width = tokens.shape
    R = w_query.shape[0]
    local_kv = w_key.shape[1] // HD
    local_heads = w_query.shape[1] // HD
    A = 2 * local_kv
    Y = n_seq // A
    hpg = local_heads // A
    slots = block_order.shape[0] // n_seq
    blk = rows // slots
    T = n_seq * rows
    QW = hpg * HD
    frequency = 500000.0 ** (-jnp.arange(HD // 2, dtype=jnp.float32) / (HD // 2))
    freq = jnp.concatenate([frequency, frequency])[None, :]
    sizes = (X, A, Y, rows, R, hpg, slots, blk, T)
    dma = pltpu.SemaphoreType.DMA
    smem = pl.BlockSpec(memory_space=pltpu.SMEM)
    vmem = pl.BlockSpec(memory_space=pltpu.VMEM)
    anywhere = pl.BlockSpec(memory_space=pl.ANY)
    attended, other = pl.pallas_call(
        functools.partial(attend_kernel, sizes),
        out_shape=(
            jax.ShapeDtypeStruct((rows, local_heads * HD), jnp.bfloat16),
            jax.ShapeDtypeStruct(prev_kv.shape, prev_kv.dtype),
        ),
        in_specs=[smem, smem, vmem, vmem] + [anywhere] * 5,
        out_specs=(vmem, anywhere),
        scratch_shapes=[
            pltpu.VMEM((A, rows, width), jnp.bfloat16),
            pltpu.VMEM((width, QW + HD), jnp.bfloat16),
            pltpu.VMEM((A, rows, width), jnp.bfloat16),
            pltpu.VMEM((A, rows, QW), jnp.bfloat16),
            pltpu.VMEM((2, n_seq, rows, HD), jnp.bfloat16),
            pltpu.VMEM((2, A, rows, HD), jnp.float32),
            pltpu.VMEM((A, rows, QW), jnp.bfloat16),
            dma((4,)),
            dma((2, A)),
            dma((A,)),
            dma((A,)),
            dma((A, X * Y)),
            dma((A, Y, X)),
            dma((2,)),
            dma((A,)),
            dma((A,)),
            dma((A,)),
            dma((A,)),
            dma((2,)),
            dma((A, 2 * Y)),
            dma((2, A, Y)),
            dma((A,)),
            dma((A,)),
        ],
        compiler_params=pltpu.CompilerParams(
            collective_id=0, has_side_effects=True
        ),
    )(
        block_order,
        block_docs,
        freq,
        norm_gain[None, :],
        tokens,
        w_query,
        w_key,
        w_value,
        prev_kv,
    )
    d = lax.axis_index("dec")
    head_count = prev_kv.shape[2]
    mine = head_count // 2
    owner = lax.dynamic_slice_in_dim(head_owner, d * mine, mine)
    both = jnp.concatenate(
        [jnp.where(d == 0, prev_kv, other), jnp.where(d == 0, other, prev_kv)], 0
    )
    picks = []
    for s in range(mine):
        chosen = both[:, :, 0]
        for j in range(1, head_count):
            chosen = jnp.where(owner[s] == j, both[:, :, j], chosen)
        picks.append(chosen)
    return attended, jnp.stack(picks, 2)


def solution(mesh):
    in_specs = (
        P(("groups", "seq"), None),
        P(),
        P("seq", "dec"),
        P("seq", "dec"),
        P("seq", "dec"),
        P("groups"),
        P("groups"),
        P("groups"),
        P(("groups", "seq", "dec"), None, None, None),
    )
    out_specs = (P(("groups", "seq"), "dec"), P(("groups", "seq"), None, "dec", None))
    X = mesh.shape["groups"]
    n_seq = mesh.shape["seq"]

    def per_device(tokens, norm_gain, w_query, w_key, w_value, *rest):
        A = 2 * (w_key.shape[1] // HD)
        heads = w_query.shape[1] // HD
        fits = (
            mesh.shape["dec"] == 2
            and A & (A - 1) == 0
            and n_seq % A == 0
            and heads % A == 0
            and w_query.shape[0] % (16 * X) == 0
            and tokens.shape[0] % 32 == 0
        )
        plan = functools.partial(column_plan, X) if fits else general_plan
        return plan(tokens, norm_gain, w_query, w_key, w_value, *rest)

    return jax.shard_map(
        per_device, mesh=mesh, in_specs=in_specs, out_specs=out_specs, check_vma=False
    )
```

```python
import functools
import math

import jax
import jax.numpy as jnp
from jax import lax
from jax.experimental import pallas as pl
from jax.experimental.pallas import tpu as pltpu
from jax.sharding import PartitionSpec as P

HD = 128


def rotate(values, positions):
    half_width = values.shape[-1] // 2
    frequency = 500000.0 ** (-jnp.arange(half_width, dtype=jnp.float32) / half_width)
    angles = positions[:, None].astype(jnp.float32) * frequency[None, :]
    cosines = jnp.cos(angles)[:, None, :]
    sine_terms = jnp.sin(angles)[:, None, :]
    lower_half = values[..., :half_width]
    upper_half = values[..., half_width:]
    return jnp.concatenate(
        [
            lower_half * cosines - upper_half * sine_terms,
            upper_half * cosines + lower_half * sine_terms,
        ],
        -1,
    )


def general_plan(
    tokens, norm_gain, w_query, w_key, w_value, block_order, block_docs, head_owner, prev_kv
):
    rows_dev = tokens.shape[0]
    block_rows = rows_dev // 2
    inputs = tokens.astype(jnp.float32)
    normed = (
        inputs * lax.rsqrt(jnp.mean(inputs * inputs, -1, keepdims=True) + 1e-05) * norm_gain
    ).astype(jnp.bfloat16)

    def add_piece(piece):
        return jnp.dot(normed, piece, preferred_element_type=jnp.float32)

    pieces = (
        lax.all_gather(w_query, "seq", axis=0, tiled=True),
        lax.all_gather(w_key, "seq", axis=0, tiled=True),
        lax.all_gather(w_value, "seq", axis=0, tiled=True),
    )
    query_full, key_full, value_full = tuple((add_piece(piece) for piece in pieces))
    total_rows = rows_dev * lax.axis_size("seq")
    row_ids = jnp.arange(total_rows, dtype=jnp.int32)
    natural = jnp.take(block_order, row_ids // block_rows)
    pos_all = natural * block_rows + row_ids % block_rows
    doc_all = jnp.take(block_docs, natural)
    offset = lax.axis_index("seq") * rows_dev
    my_pos = lax.dynamic_slice_in_dim(pos_all, offset, rows_dev)
    my_doc = lax.dynamic_slice_in_dim(doc_all, offset, rows_dev)
    local_kv = key_full.shape[1] // HD
    local_heads = query_full.shape[1] // HD
    group_size = local_heads // local_kv
    queries = rotate(query_full.reshape(rows_dev, local_heads, HD), my_pos).astype(jnp.bfloat16)
    query_groups = queries.reshape(rows_dev, local_kv, group_size, HD).transpose(1, 2, 0, 3)
    key_rows = (
        rotate(key_full.reshape(rows_dev, local_kv, HD), my_pos)
        .astype(jnp.bfloat16)
        .reshape(rows_dev, local_kv * HD)
    )
    value_rows = value_full.astype(jnp.bfloat16)
    scale = 1.0 / math.sqrt(HD)
    start_max = jnp.full((local_kv, group_size, rows_dev, 1), -jnp.inf, jnp.float32)
    start_sum = jnp.zeros((local_kv, group_size, rows_dev, 1), jnp.float32)
    start_weighted = jnp.zeros((local_kv, group_size, rows_dev, HD), jnp.float32)
    key_piece = lax.all_gather(key_rows, "seq", axis=0, tiled=True)
    value_piece = lax.all_gather(value_rows, "seq", axis=0, tiled=True)
    count = key_piece.shape[0]
    allowed = (pos_all[None, :] <= my_pos[:, None]) & (doc_all[None, :] == my_doc[:, None])

    def update(state):
        running_max, running_sum, weighted = state
        scores = (
            jnp.einsum(
                "ghtd,sgd->ghts",
                query_groups,
                key_piece.reshape(count, local_kv, HD),
                preferred_element_type=jnp.float32,
            )
            * scale
        )
        scores = jnp.where(allowed, scores, -jnp.inf)
        new_max = jnp.max(scores, -1, keepdims=True)
        shift_by = jnp.where(new_max == -jnp.inf, 0.0, new_max)
        weights = jnp.exp(scores - shift_by)
        rescale = jnp.exp(running_max - shift_by)
        running_sum = running_sum * rescale + jnp.sum(weights, -1, keepdims=True)
        weighted = weighted * rescale + jnp.einsum(
            "ghts,sgd->ghtd",
            weights.astype(jnp.bfloat16),
            value_piece.reshape(count, local_kv, HD),
            preferred_element_type=jnp.float32,
        )
        return (new_max, running_sum, weighted)

    final_max, final_sum, final_weighted = lax.cond(
        jnp.any(allowed), update, lambda state: state, (start_max, start_sum, start_weighted)
    )
    attended = (
        (final_weighted / final_sum)
        .transpose(2, 0, 1, 3)
        .reshape(rows_dev, local_heads * HD)
        .astype(jnp.bfloat16)
    )
    head_count = prev_kv.shape[2]
    selector = (head_owner[:, None] == jnp.arange(head_count, dtype=jnp.int32)[None, :]).astype(
        jnp.bfloat16
    )
    ordered = jnp.einsum(
        "tcjd,sj->tcsd", prev_kv, selector, preferred_element_type=jnp.float32
    ).astype(jnp.bfloat16)
    decode_cache = lax.all_to_all(ordered, "dec", split_axis=2, concat_axis=0, tiled=True)
    return (attended, decode_cache)


def attend_kernel(
    sizes,
    order_ref,
    docs_ref,
    freq_ref,
    gain_ref,
    tok_in,
    wq_in,
    wk_in,
    wv_in,
    prev_in,
    out_ref,
    prev_out,
    tok,
    wbuf,
    normed,
    qbuf,
    kvbuf,
    csbuf,
    att,
    local_sem,
    home_send,
    homeq_recv,
    homekv_recv,
    rel_send,
    rel_recv,
    own_send,
    fwd_send,
    tok_recv,
    sib_send,
    sib_recv,
    prev_sem,
    kv_send,
    kv_recv,
    att_send,
    att_recv,
):
    X, A, Y, rows, R, hpg, slots, blk, T = sizes
    Rp = R // X
    half = rows // 2
    QW = hpg * HD
    x = lax.axis_index("groups")
    q = lax.axis_index("seq")
    d = lax.axis_index("dec")
    a = q // Y
    y = q % Y
    unit = a % 2

    def dev(x_, a_, y_, d_=None):
        return {"groups": x_, "seq": a_ * Y + y_, "dec": d if d_ is None else d_}

    def remote(src, dst, ssem, rsem, device):
        return pltpu.make_async_remote_copy(
            src_ref=src,
            dst_ref=dst,
            send_sem=ssem,
            recv_sem=rsem,
            device_id=device,
            device_id_type=pl.DeviceIdType.MESH,
        )

    sibling = dev(x, a, y, 1 - d)
    barrier = pltpu.get_barrier_semaphore()
    plane = [(i, j) for i in range(X) for j in range(Y) if (i, j) != (0, 0)]
    peers = [dev((x + i) % X, a, (y + j) % Y) for i, j in plane]
    peers += [dev(x, (a + t) % A, y) for t in range(1, A)]
    mate = a + 1 - 2 * unit
    peers += [dev(x, mate, (y + j) % Y) for j in range(1, Y)]
    peers.append(sibling)
    for peer in peers:
        pl.semaphore_signal(barrier, inc=1, device_id=peer, device_id_type=pl.DeviceIdType.MESH)
    pl.semaphore_wait(barrier, len(peers))

    def w_rows(a_, y_, x_):
        return pl.ds(pl.multiple_of((a_ * Y + y_) * R + x_ * Rp, Rp), Rp)

    part = pl.ds(pl.multiple_of(x * Rp, Rp), Rp)

    def kv_source(t):
        return wv_in if t % 2 else wk_in

    def home_copies(t):
        kv_cols = pl.ds((t // 2) * HD, HD)
        return (
            remote(
                wq_in.at[part, pl.ds(t * QW, QW)],
                wbuf.at[w_rows(a, y, x), pl.ds(0, QW)],
                home_send.at[0, t],
                homeq_recv.at[a],
                dev(x, t, y),
            ),
            remote(
                kv_source(t).at[part, kv_cols],
                wbuf.at[w_rows(a, y, x), pl.ds(QW, HD)],
                home_send.at[1, t],
                homekv_recv.at[a],
                dev(x, t, y),
            ),
        )

    def local_copies(t):
        rows_all = pl.ds(pl.multiple_of(q * R, R), R)
        return (
            pltpu.make_async_copy(
                wq_in.at[:, pl.ds(t * QW, QW)],
                wbuf.at[rows_all, pl.ds(0, QW)],
                local_sem.at[0],
            ),
            pltpu.make_async_copy(
                kv_source(t).at[:, pl.ds((t // 2) * HD, HD)],
                wbuf.at[rows_all, pl.ds(QW, HD)],
                local_sem.at[1],
            ),
        )

    for t in range(A):

        @pl.when(a == t)
        def _():
            for copy in local_copies(t):
                copy.start()

        @pl.when(a != t)
        def _():
            for copy in home_copies(t):
                copy.start()

    my_half = pl.ds(pl.multiple_of(d * half, half), half)
    other_half = pl.ds(pl.multiple_of((1 - d) * half, half), half)

    def own_push(side):
        return remote(
            tok_in.at[my_half],
            tok.at[a, my_half],
            own_send.at[side],
            tok_recv.at[a],
            dev(x, a + 1 - 2 * side, y),
        )

    @pl.when(a + 1 < A)
    def _():
        own_push(0).start()

    @pl.when(a >= 1)
    def _():
        own_push(1).start()

    own_tok = pltpu.make_async_copy(tok_in, tok.at[a], local_sem.at[2])
    own_tok.start()
    prev_copy = remote(prev_in, prev_out, prev_sem.at[0], prev_sem.at[1], sibling)
    prev_copy.start()

    def relay(t, index, i, j):
        src = wbuf.at[w_rows(t, y, x)]
        return remote(
            src,
            src,
            rel_send.at[t, index],
            rel_recv.at[t, y, x],
            dev((x + i) % X, a, (y + j) % Y),
        )

    for t in range(A):

        @pl.when(a == t)
        def _():
            for copy in local_copies(t):
                copy.wait()
            for index, (i, j) in enumerate(plane):
                if j:
                    relay(t, index, i, j).start()

    lane = lax.broadcasted_iota(jnp.int32, (rows, HD), 1)
    row_id = lax.broadcasted_iota(jnp.int32, (rows, 1), 0)

    def row_values(c, table):
        value = jnp.zeros((rows, 1), jnp.int32)
        for i in range(slots):
            entry = table(order_ref[(c * Y + y) * slots + i])
            value = jnp.where(row_id // blk == i, entry, value)
        return value

    def row_positions(c):
        return row_values(c, lambda n: n) * blk + row_id % blk

    for o in range(1, A):
        t = (a + o) % A
        src = wbuf.at[w_rows(t, y, x)]
        remote(
            wq_in.at[part, pl.ds(0, QW)],
            wbuf.at[w_rows(t, y, x), pl.ds(0, QW)],
            home_send.at[0, 0],
            homeq_recv.at[t],
            sibling,
        ).wait_recv()
        remote(
            wk_in.at[part, pl.ds(0, HD)],
            wbuf.at[w_rows(t, y, x), pl.ds(QW, HD)],
            home_send.at[1, 0],
            homekv_recv.at[t],
            sibling,
        ).wait_recv()
        for index, (i, j) in enumerate(plane):
            relay(t, index, i, j).start()

    def forward(c, to):
        return remote(
            tok.at[c, my_half],
            tok.at[c, my_half],
            fwd_send.at[c],
            tok_recv.at[c],
            dev(x, to, y),
        )

    def share(c):
        return remote(
            tok.at[c, my_half], tok.at[c, my_half], sib_send.at[c], sib_recv.at[c], sibling
        )

    def token_step(s):
        @pl.when(a >= s)
        def _():
            c = a - s
            forward(c, a).wait_recv()

            @pl.when(a + 1 < A)
            def _():
                forward(c, a + 1).start()

            share(c).start()

        @pl.when(a + s < A)
        def _():
            c = a + s
            forward(c, a).wait_recv()

            @pl.when(a >= 1)
            def _():
                forward(c, a - 1).start()

            share(c).start()

    def pick(s):
        value, bit = 0, 1
        while bit < A:
            value = value + bit * ((a // bit + s // bit) % 2)
            bit *= 2
        return value

    def kv_peer(dy, da):
        return dev(x, a - unit + (unit + da) % 2, (y + dy) % Y)

    kv_plan = [(dy, da) for dy in range(Y) for da in range(2) if (dy, da) != (0, 0)]

    def kv_push(s, c, index, dy, da):
        src = kvbuf.at[unit, c * Y + y]
        return remote(src, src, kv_send.at[s, index], kv_recv.at[unit, c, y], kv_peer(dy, da))

    def normalize(s):
        c = pick(s)
        if s == 0:
            own_tok.wait()
        else:
            other = tok.at[c, other_half]
            remote(other, other, sib_send.at[c], sib_recv.at[c], sibling).wait_recv()

        def block(i, carry):
            span = pl.ds(pl.multiple_of(i * 16, 16), 16)
            inputs = tok[c, span].astype(jnp.float32)
            mean = jnp.mean(inputs * inputs, -1, keepdims=True)
            normed[c, span] = (inputs * lax.rsqrt(mean + 1e-05) * gain_ref[...]).astype(
                jnp.bfloat16
            )
            return carry

        lax.fori_loop(0, rows // 16, block, 0, unroll=2)

    def project(s, carry):
        c = pick(s)
        cosine = csbuf[0, c]
        sine = csbuf[1, c]

        def turn(v):
            return v * cosine + pltpu.roll(v, HD // 2, 1) * sine

        raw = jnp.dot(normed[c], wbuf[:, QW:], preferred_element_type=jnp.float32)
        kvbuf[unit, c * Y + y] = jnp.where(unit == 0, turn(raw), raw).astype(jnp.bfloat16)
        product = jnp.dot(normed[c], wbuf[:, :QW], preferred_element_type=jnp.float32)
        for index, (dy, da) in enumerate(kv_plan):
            kv_push(s, c, index, dy, da).start()
        for h in range(hpg):
            qbuf[c, :, h * HD : (h + 1) * HD] = turn(product[:, h * HD : (h + 1) * HD]).astype(
                jnp.bfloat16
            )
        return carry

    step_angle = (row_id % blk).astype(jnp.float32) * freq_ref[...]
    step_cos = jnp.cos(step_angle)
    step_sin = jnp.sin(step_angle)
    sign = jnp.where(lane < HD // 2, -1.0, 1.0)
    entry_id = lax.broadcasted_iota(jnp.int32, (A * slots, 1), 0)
    entries = jnp.zeros((A * slots, 1), jnp.int32)
    for c in range(A):
        for i in range(slots):
            entries = jnp.where(
                entry_id == c * slots + i, order_ref[(c * Y + y) * slots + i], entries
            )
    base_angle = (entries * blk).astype(jnp.float32) * freq_ref[...]
    base_cos = jnp.cos(base_angle)
    base_sin = jnp.sin(base_angle)
    for c in range(A):
        row_cos = jnp.broadcast_to(base_cos[c * slots : c * slots + 1], (rows, HD))
        row_sin = jnp.broadcast_to(base_sin[c * slots : c * slots + 1], (rows, HD))
        for i in range(1, slots):
            k = c * slots + i
            row_cos = jnp.where(row_id // blk == i, base_cos[k : k + 1], row_cos)
            row_sin = jnp.where(row_id // blk == i, base_sin[k : k + 1], row_sin)
        csbuf[0, c] = row_cos * step_cos - row_sin * step_sin
        csbuf[1, c] = (row_sin * step_cos + row_cos * step_sin) * sign

    normalize(0)
    for s in range(1, A - 1):
        token_step(s)
        normalize(s)
    for o in range(A):
        t = (a + o) % A
        for i, j in plane:
            if o or j:
                src = wbuf.at[w_rows(t, (y + j) % Y, (x + i) % X)]
                remote(
                    src,
                    src,
                    rel_send.at[0, 0],
                    rel_recv.at[t, (y + j) % Y, (x + i) % X],
                    sibling,
                ).wait_recv()

    lax.fori_loop(0, A - 1, project, 0)
    token_step(A - 1)
    normalize(A - 1)
    project(A - 1, 0)

    for s in range(A):
        c = pick(s)
        for dy, da in kv_plan:
            u = (unit + da) % 2
            dst = kvbuf.at[u, c * Y + (y + dy) % Y]
            remote(
                dst, dst, kv_send.at[0, 0], kv_recv.at[u, c, (y + dy) % Y], sibling
            ).wait_recv()

    key_id = lax.broadcasted_iota(jnp.int32, (1, T), 1)
    key_pos = jnp.zeros((1, T), jnp.int32)
    key_doc = jnp.zeros((1, T), jnp.int32)
    for i in range(T // blk):
        here = key_id // blk == i
        natural = order_ref[i]
        key_pos = jnp.where(here, natural * blk, key_pos)
        key_doc = jnp.where(here, docs_ref[natural], key_doc)
    key_pos = key_pos + key_id % blk
    scale = 1.0 / math.sqrt(HD)
    out_cols = pl.ds(pl.multiple_of(a * QW, QW), QW)

    def att_push(s, c):
        return remote(
            att.at[c], out_ref.at[:, out_cols], att_send.at[s], att_recv.at[a], dev(x, c, y)
        )

    def attend(s, carry):
        c = pick(A - 1 - s)
        allowed = (key_pos <= row_positions(c)) & (
            key_doc == row_values(c, lambda n: docs_ref[n])
        )
        keys = kvbuf[0].reshape(T, HD)
        values = kvbuf[1].reshape(T, HD)
        for h in range(hpg):
            scores = (
                lax.dot_general(
                    qbuf[c, :, h * HD : (h + 1) * HD],
                    keys,
                    (((1,), (1,)), ((), ())),
                    preferred_element_type=jnp.float32,
                )
                * scale
            )
            scores = jnp.where(allowed, scores, -jnp.inf)
            weights = jnp.exp(scores - jnp.max(scores, -1, keepdims=True))
            total = jnp.sum(weights, -1, keepdims=True)
            weighted = jnp.dot(
                weights.astype(jnp.bfloat16), values, preferred_element_type=jnp.float32
            )
            att[c, :, h * HD : (h + 1) * HD] = (weighted / total).astype(jnp.bfloat16)

        @pl.when(s < A - 1)
        def _():
            att_push(s, c).start()

        return carry

    lax.fori_loop(0, A, attend, 0)
    own_out = pltpu.make_async_copy(att.at[a], out_ref.at[:, out_cols], local_sem.at[3])
    own_out.start()

    for t in range(A):

        @pl.when(a != t)
        def _():
            for copy in home_copies(t):
                copy.wait_send()
            for index, (i, j) in enumerate(plane):
                relay(t, index, i, j).wait_send()

        @pl.when(a == t)
        def _():
            for index, (i, j) in enumerate(plane):
                if j:
                    relay(t, index, i, j).wait_send()

    @pl.when(a + 1 < A)
    def _():
        own_push(0).wait_send()

    @pl.when(a >= 1)
    def _():
        own_push(1).wait_send()

    for s in range(1, A):

        @pl.when(a >= s)
        def _():
            share(a - s).wait_send()

            @pl.when(a + 1 < A)
            def _():
                forward(a - s, a + 1).wait_send()

        @pl.when(a + s < A)
        def _():
            share(a + s).wait_send()

            @pl.when(a >= 1)
            def _():
                forward(a + s, a - 1).wait_send()

    for s in range(A):
        for index, (dy, da) in enumerate(kv_plan):
            kv_push(s, pick(s), index, dy, da).wait_send()
    prev_copy.wait()
    own_out.wait()
    for s in range(A - 1):
        att_push(s, pick(A - 1 - s)).wait_send()
    for o in range(1, A):
        t = (a + o) % A
        cols = pl.ds(pl.multiple_of(t * QW, QW), QW)
        remote(
            att.at[0], out_ref.at[:, cols], att_send.at[0], att_recv.at[t], sibling
        ).wait_recv()


def column_plan(
    X, tokens, norm_gain, w_query, w_key, w_value, block_order, block_docs, head_owner, prev_kv
):
    n_seq = lax.axis_size("seq")
    rows, width = tokens.shape
    R = w_query.shape[0]
    local_kv = w_key.shape[1] // HD
    local_heads = w_query.shape[1] // HD
    A = 2 * local_kv
    Y = n_seq // A
    hpg = local_heads // A
    slots = block_order.shape[0] // n_seq
    blk = rows // slots
    T = n_seq * rows
    QW = hpg * HD
    frequency = 500000.0 ** (-jnp.arange(HD // 2, dtype=jnp.float32) / (HD // 2))
    freq = jnp.concatenate([frequency, frequency])[None, :]
    sizes = (X, A, Y, rows, R, hpg, slots, blk, T)
    dma = pltpu.SemaphoreType.DMA
    smem = pl.BlockSpec(memory_space=pltpu.SMEM)
    vmem = pl.BlockSpec(memory_space=pltpu.VMEM)
    anywhere = pl.BlockSpec(memory_space=pl.ANY)
    attended, other = pl.pallas_call(
        functools.partial(attend_kernel, sizes),
        out_shape=(
            jax.ShapeDtypeStruct((rows, local_heads * HD), jnp.bfloat16),
            jax.ShapeDtypeStruct(prev_kv.shape, prev_kv.dtype),
        ),
        in_specs=[smem, smem, vmem, vmem] + [anywhere] * 5,
        out_specs=(vmem, anywhere),
        scratch_shapes=[
            pltpu.VMEM((A, rows, width), jnp.bfloat16),
            pltpu.VMEM((width, QW + HD), jnp.bfloat16),
            pltpu.VMEM((A, rows, width), jnp.bfloat16),
            pltpu.VMEM((A, rows, QW), jnp.bfloat16),
            pltpu.VMEM((2, n_seq, rows, HD), jnp.bfloat16),
            pltpu.VMEM((2, A, rows, HD), jnp.float32),
            pltpu.VMEM((A, rows, QW), jnp.bfloat16),
            dma((4,)),
            dma((2, A)),
            dma((A,)),
            dma((A,)),
            dma((A, X * Y)),
            dma((A, Y, X)),
            dma((2,)),
            dma((A,)),
            dma((A,)),
            dma((A,)),
            dma((A,)),
            dma((2,)),
            dma((A, 2 * Y)),
            dma((2, A, Y)),
            dma((A,)),
            dma((A,)),
        ],
        compiler_params=pltpu.CompilerParams(
            collective_id=0, has_side_effects=True
        ),
    )(
        block_order,
        block_docs,
        freq,
        norm_gain[None, :],
        tokens,
        w_query,
        w_key,
        w_value,
        prev_kv,
    )
    d = lax.axis_index("dec")
    head_count = prev_kv.shape[2]
    mine = head_count // 2
    owner = lax.dynamic_slice_in_dim(head_owner, d * mine, mine)
    both = jnp.concatenate(
        [jnp.where(d == 0, prev_kv, other), jnp.where(d == 0, other, prev_kv)], 0
    )
    picks = []
    for s in range(mine):
        chosen = both[:, :, 0]
        for j in range(1, head_count):
            chosen = jnp.where(owner[s] == j, both[:, :, j], chosen)
        picks.append(chosen)
    return attended, jnp.stack(picks, 2)


def solution(mesh):
    in_specs = (
        P(("groups", "seq"), None),
        P(),
        P("seq", "dec"),
        P("seq", "dec"),
        P("seq", "dec"),
        P("groups"),
        P("groups"),
        P("groups"),
        P(("groups", "seq", "dec"), None, None, None),
    )
    out_specs = (P(("groups", "seq"), "dec"), P(("groups", "seq"), None, "dec", None))
    X = mesh.shape["groups"]
    n_seq = mesh.shape["seq"]

    def per_device(tokens, norm_gain, w_query, w_key, w_value, *rest):
        A = 2 * (w_key.shape[1] // HD)
        heads = w_query.shape[1] // HD
        fits = (
            mesh.shape["dec"] == 2
            and A & (A - 1) == 0
            and n_seq % A == 0
            and heads % A == 0
            and w_query.shape[0] % (16 * X) == 0
            and tokens.shape[0] % 32 == 0
        )
        plan = functools.partial(column_plan, X) if fits else general_plan
        return plan(tokens, norm_gain, w_query, w_key, w_value, *rest)

    return jax.shard_map(
        per_device, mesh=mesh, in_specs=in_specs, out_specs=out_specs, check_vma=False
    )
```
